32 devices in a mesh: rep: 2 (over x), zero: 16 (over z, y, core).
Axes of the slice: x: 2, y: 2, z: 4, core: 2. Of those that a mesh axis runs over, the one named last changes fastest.
Arguments:
- acts: bfloat16 [256, 8192], P('rep', 'zero'), may hold values from -6 to 6
- grads_out: bfloat16 [256, 8192], P('rep', 'zero'), may hold values from -12 to 12
- act_inverse: bfloat16 [8192, 8192], P('zero'), as said below
- grad_inverse: bfloat16 [8192, 8192], P('zero'), as said below
Outputs:
- precond: float32 [8192, 8192], P('zero')
The draws below stay inside these ranges and needn't reach their ends.
Inputs may be any that keep to these rules, and one draw needn't show every extreme that they name: act_inverse is symmetric. grad_inverse is symmetric.
All inputs are finite; a program needn't handle non-finite values.
Results may differ from the reference program's by a relative error of at most 0.004.
Values may be sent and summed in bfloat16 or wider, within the bound.
A program may use at most 128 MiB of HBM per device.

```python
import math
import jax
import jax.numpy as jnp
from jax import lax

D = 8192
TOKENS = 256


def make_inverse(key):
    key_raw, key_diag = jax.random.split(key, 2)
    raw = jax.random.normal(key_raw, (D, D), jnp.float32) / math.sqrt(D)
    matrix = (raw + raw.T) * 0.5
    diagonal = jax.random.uniform(key_diag, (D,), jnp.float32, 1.5, 3.0)
    matrix = matrix + jnp.diag(diagonal)
    return matrix.astype(jnp.bfloat16)


def draw_act_inverse(key, part):
    return make_inverse(jax.random.fold_in(key, 11))


def draw_grad_inverse(key, part):
    return make_inverse(jax.random.fold_in(key, 23))


def shard_levels(key, dims, shards, smallest, largest):
    loudness = 1.0
    for dim, shards_of in shards:
        draws = jax.random.uniform(jax.random.fold_in(jax.random.fold_in(key, 6), dim), (shards_of,), jnp.float32, smallest / len(shards), largest / len(shards))
        loudness = loudness * jnp.repeat(jnp.exp(draws), dims[dim] // shards_of).reshape((-1,) + (1,) * (len(dims) - 1 - dim))
    return loudness


def scatter_about(stream_key, shape, scale, bound, cuts=(), held_as=jnp.bfloat16):
    gain = shard_levels(stream_key, shape, cuts, -0.22, 0.18) if cuts else 1.0
    entries = jax.random.normal(stream_key, shape, jnp.float32) * scale * gain
    return jnp.minimum(jnp.maximum(entries, -bound), bound).astype(held_as)


def setup_inputs(seed: int = 0) -> dict:
    splits = jax.random.split(jax.random.key(seed), 5)
    acts = scatter_about(splits[0], (TOKENS, D), 1.0, 6.0, ((0, 2), (1, 16)))
    grads_out = scatter_about(splits[1], (TOKENS, D), 2.0, 12.0, ((0, 2), (1, 16)))
    act_inverse = draw_act_inverse(jax.random.fold_in(splits[4], 71), 0)
    grad_inverse = draw_grad_inverse(jax.random.fold_in(splits[4], 71), 0)
    return {"acts": acts, "grads_out": grads_out, "act_inverse": act_inverse, "grad_inverse": grad_inverse}


def reference(acts, grads_out, act_inverse, grad_inverse):
    act_pre = jnp.dot(acts, act_inverse, preferred_element_type=jnp.float32).astype(jnp.bfloat16)
    grad_pre = jnp.dot(grads_out, grad_inverse, preferred_element_type=jnp.float32).astype(jnp.bfloat16)
    summed = lax.dot_general(grad_pre, act_pre, (((0,), (0,)), ((), ())), preferred_element_type=jnp.float32)
    return summed / jnp.float32(TOKENS)
```

```python
import functools

import jax
import jax.numpy as jnp
from jax import lax
from jax.experimental import pallas as pl
from jax.experimental.pallas import tpu as pltpu
from jax.sharding import PartitionSpec as P

NT = (((1,), (1,)), ((), ()))


def gathered(acts, grads_out, act_inverse, grad_inverse):
    group = acts.shape[0]
    total_tokens = group * lax.axis_size("rep")
    both = lax.all_gather(jnp.concatenate([acts, grads_out], 0), "zero", axis=1, tiled=True)
    act_own = lax.dot_general(
        both[:group], act_inverse, NT, preferred_element_type=jnp.float32
    ).astype(jnp.bfloat16)
    act_pre = lax.all_gather(act_own, ("rep", "zero"), axis=0)
    grad_own = lax.dot_general(
        both[group:], grad_inverse, NT, preferred_element_type=jnp.float32
    ).astype(jnp.bfloat16)
    grad_pre = lax.all_gather(grad_own, "rep", axis=0, tiled=True)
    zero = lax.axis_size("zero")
    act_pre = act_pre.reshape(-1, zero, group, act_own.shape[1]).transpose(0, 2, 1, 3)
    act_pre = act_pre.reshape(total_tokens, -1)
    summed = lax.dot_general(
        grad_pre, act_pre, (((0,), (0,)), ((), ())), preferred_element_type=jnp.float32
    )
    return summed / jnp.float32(total_tokens)


MESH = pl.DeviceIdType.MESH

PIECES = (4, 2, 2)
SWAPPED = (0, 0, 1)
ROUND_Y, ROUND_Z = 2, 1
KERNEL_VMEM = 46137344


ORDERS = {4: [('own', 0), ('near', 0, 0, 0, 0, 1), ('near', 0, 0, 0, 0, 2), ('near', 0, 1, 0, 0, 1), ('near', 0, 1, 0, 1, 0), ('near', 0, 1, 0, 0, 2), ('near', 0, 3, 0, 0, 1), ('near', 0, 3, 0, 0, 2), ('near', 0, 2, 0, 0, 1), ('near', 0, 0, 0, 1, 1), ('near', 0, 1, 0, 0, 3), ('near', 0, 0, 0, 1, 0), ('near', 0, 0, 0, 0, 3), ('near', 0, 2, 0, 0, 2), ('near', 0, 1, 0, 1, 1), ('near', 0, 2, 0, 1, 0), ('near', 0, 3, 0, 0, 3), ('near', 0, 3, 0, 1, 1), ('near', 0, 3, 0, 1, 0), ('near', 0, 2, 0, 0, 3), ('partner', 0, 0, 0, 2), ('own', 1), ('near', 0, 1, 0, 1, 2), ('near', 0, 2, 0, 1, 1), ('partner', 0, 0, 0, 1), ('near', 0, 3, 0, 1, 2), ('partner', 0, 0, 1, 1), ('near', 0, 0, 0, 1, 2), ('near', 0, 2, 0, 1, 2), ('partner', 0, 0, 0, 0), ('partner', 0, 0, 1, 0), ('near', 1, 0, 0, 0, 2), ('partner', 0, 0, 0, 3), ('near', 0, 3, 0, 1, 3), ('near', 0, 0, 0, 1, 3), ('near', 0, 1, 0, 1, 3), ('near', 0, 2, 0, 1, 3), ('partner', 1, 0, 0, 0), ('partner', 0, 0, 1, 2), ('near', 1, 1, 0, 0, 2), ('partner', 0, 0, 1, 3), ('own', 2), ('near', 2, 0, 0, 0, 2), ('near', 1, 0, 0, 0, 1), ('near', 2, 1, 0, 0, 2), ('near', 2, 1, 0, 1, 0), ('near', 1, 1, 0, 1, 0), ('near', 2, 0, 0, 0, 1), ('near', 1, 1, 0, 0, 1), ('near', 2, 0, 0, 1, 2), ('near', 2, 0, 0, 1, 0), ('near', 1, 1, 0, 1, 2), ('near', 2, 1, 0, 0, 1), ('near', 1, 0, 0, 0, 3), ('partner', 1, 0, 0, 2), ('near', 2, 1, 0, 1, 2), ('near', 2, 0, 0, 1, 1), ('near', 1, 0, 0, 1, 0), ('near', 2, 0, 1, 0, 0), ('near', 2, 1, 0, 1, 1), ('near', 1, 0, 0, 1, 2), ('partner', 1, 0, 1, 0), ('near', 1, 1, 0, 0, 3), ('near', 1, 0, 0, 1, 1), ('partner', 1, 0, 0, 1), ('near', 1, 1, 0, 1, 1), ('near', 2, 0, 0, 0, 3), ('near', 2, 1, 0, 0, 3), ('near', 2, 1, 1, 0, 1), ('partner', 1, 0, 1, 1), ('near', 2, 1, 1, 0, 0), ('near', 2, 0, 1, 0, 1), ('near', 2, 1, 0, 1, 3), ('near', 1, 1, 0, 1, 3), ('near', 1, 0, 0, 1, 3), ('near', 2, 0, 1, 1, 1), ('near', 2, 0, 1, 0, 3), ('near', 2, 0, 0, 1, 3), ('partner', 1, 0, 1, 2), ('partner', 1, 0, 1, 3), ('partner', 1, 0, 0, 3), ('near', 2, 0, 1, 1, 0), ('near', 2, 1, 1, 1, 2), ('near', 2, 0, 1, 0, 2), ('near', 2, 1, 1, 0, 2), ('near', 2, 1, 1, 1, 0), ('swap', 1), ('near', 2, 1, 1, 1, 3), ('near', 2, 0, 1, 1, 2), ('near', 2, 1, 1, 1, 1), ('near', 2, 1, 1, 0, 3), ('near', 2, 0, 1, 1, 3), ('partner', 2, 0, 0, 0), ('partner', 2, 0, 0, 1), ('partner', 2, 0, 0, 2), ('partner', 2, 0, 0, 3), ('partner', 2, 0, 1, 0), ('partner', 2, 0, 1, 1), ('partner', 2, 0, 1, 2), ('partner', 2, 0, 1, 3), ('partner', 2, 1, 0, 0), ('partner', 2, 1, 0, 1), ('partner', 2, 1, 0, 2), ('partner', 2, 1, 0, 3), ('partner', 2, 1, 1, 0), ('partner', 2, 1, 1, 1), ('partner', 2, 1, 1, 2), ('partner', 2, 1, 1, 3)]}


def schedule(outer):
    return ORDERS[outer]


def nearest_first(outer):
    rows = []
    for z in range(outer):
        others = [q for q in range(outer) if q != z]
        others.sort(key=lambda q: (abs(q - z), q if 2 * z < outer else -q))
        rows.append([z] + others)
    return rows


def hops(kind, unit, r, yy, j):
    by_y, by_z = unit < ROUND_Y, unit < ROUND_Z
    if r == 1:
        if yy == 0 and j == 0:
            return ["y"] * by_y + ["up", "down"] * by_z
        return []
    ways = []
    if kind == 2:
        if yy == 1 and j == 0:
            ways += ["x"] * (not by_y)
        elif yy == 0 and j in (1, 2) and by_z:
            ways += ["x far"] * (j == 2)
        else:
            ways += ["x"]
    late = unit >= PIECES[kind] - SWAPPED[kind]
    if yy == 0 or late:
        ways += ["up", "down"] if j == 0 else ["on"]
    if yy == 0 and (j == 0 or not late):
        ways += ["y"]
    return ways


def sends_of(order):
    count, seen = 0, {}
    for what, kind, *rest in order:
        if what == "own":
            count += 1 + sum(len(hops(kind, unit, 0, 0, 0)) for unit in range(PIECES[kind]))
        elif what == "near":
            key = (kind, *rest[1:])
            seen[key] = seen.get(key, 0) + 1
            count += len(hops(kind, *rest)) + (seen[key] == PIECES[kind])
    return count


def gather_kernel(
    outer, order, acts, grads, a_hbm, g_hbm, pre, grad_pre,
    a_rows, g_rows, held, acc_a, acc_g,
    w_sem, send_sem, recv, recv_pre, x_recv, own_sem,
):
    group, width = acts.shape
    zero = outer * 4
    rep = lax.axis_index("rep")
    me = lax.axis_index("zero")
    z, y, c = me // 4, (me // 2) % 2, me % 2

    own = [
        pltpu.make_async_copy(acts, held.at[0, me], own_sem.at[0]),
        pltpu.make_async_copy(grads, held.at[1, me], own_sem.at[1]),
    ]
    loads = [
        pltpu.make_async_copy(a_hbm, a_rows, w_sem.at[0]),
        pltpu.make_async_copy(g_hbm, g_rows, w_sem.at[1]),
    ]
    own[0].start()
    own[1].start()
    loads[0].start()

    x_peer = (1 - rep, me)
    y_peer = (rep, z * 4 + (1 - y) * 2 + c)
    c_peer = (rep, z * 4 + y * 2 + 1 - c)
    has_up, has_down = z < outer - 1, z > 0

    def z_peer(to):
        return (rep, to * 4 + y * 2 + c)

    barrier = pltpu.get_barrier_semaphore()

    def greet(peer):
        pl.semaphore_signal(barrier, inc=1, device_id=peer, device_id_type=MESH)

    for peer in (x_peer, y_peer, c_peer):
        greet(peer)
    pl.when(has_up)(lambda: greet(z_peer(z + 1)))
    pl.when(has_down)(lambda: greet(z_peer(z - 1)))
    pl.semaphore_wait(barrier, 3 + has_up.astype(jnp.int32) + has_down.astype(jnp.int32))

    table = nearest_first(outer)
    at_z = []
    for j in range(outer):
        value = jnp.int32(table[0][j])
        for q in range(1, outer):
            value = jnp.where(z == q, table[q][j], value)
        at_z.append(value)

    def block_of(kind, r, yy, j, other=False):
        cc = 1 - c if other else c
        block = at_z[j] * 4 + ((y + yy) % 2) * 2 + cc
        if kind == 2:
            block += ((rep + r) % 2) * zero
        return block

    def view(kind, block, unit=None):
        ref = pre.at[block] if kind == 2 else held.at[kind, block]
        if unit is None:
            return ref
        rows = group // PIECES[kind]
        return ref.at[pl.ds(unit * rows, rows)]

    def landing(kind, block, unit):
        return recv_pre.at[block, unit] if kind == 2 else recv.at[kind, block, unit]

    sent = []

    def send(ref, peer, arrival, when=None):
        copy = pltpu.make_async_remote_copy(
            src_ref=ref, dst_ref=ref,
            send_sem=send_sem.at[len(sent)], recv_sem=arrival,
            device_id=peer, device_id_type=MESH,
        )
        sent.append((copy, when))
        if when is None:
            copy.start()
        else:
            pl.when(when)(copy.start)

    def forward(kind, unit, r, yy, j):
        block = block_of(kind, r, yy, j)
        ref, arrival = view(kind, block, unit), landing(kind, block, unit)
        onward = jnp.where(at_z[j] < z, z + 1, z - 1)
        ways = {
            "x": (x_peer, None),
            "x far": (x_peer, jnp.abs(at_z[j] - z) > 1),
            "y": (y_peer, None),
            "up": (z_peer(z + 1), has_up),
            "down": (z_peer(z - 1), has_down),
            "on": (z_peer(onward), (onward >= 0) & (onward < outer)),
        }
        for way in hops(kind, unit, r, yy, j):
            peer, when = ways[way]
            send(ref, peer, arrival, when)

    def to_partner(kind, r, yy, j):
        block = block_of(kind, r, yy, j)
        send(view(kind, block), c_peer, landing(kind, block, 0))

    begun = [False, False]

    def add(kind, block):
        value = held[kind, block]
        columns = pl.ds(pl.multiple_of(block * width, width), width)
        if kind == 0:
            acc, term = acc_a, lax.dot_general(
                value, a_rows[:, columns], NT, preferred_element_type=jnp.float32
            )
        else:
            acc, term = acc_g, lax.dot_general(
                g_rows[:, columns], value, NT, preferred_element_type=jnp.float32
            )
        if begun[kind]:
            acc[...] += term
        else:
            acc[...] = term
            begun[kind] = True

    def wait(ref, arrival):
        pltpu.make_async_copy(ref, ref, arrival).wait()

    mine = rep * zero + me
    arrived = {}
    swap = pltpu.make_async_remote_copy(
        src_ref=grad_pre.at[rep], dst_ref=grad_pre.at[rep],
        send_sem=own_sem.at[2], recv_sem=x_recv,
        device_id=x_peer, device_id_type=MESH,
    )
    for step in order:
        what, kind = step[0], step[1]
        if what == "own":
            if kind == 2:
                pre[mine] = acc_a[...].astype(jnp.bfloat16)
            else:
                own[kind].wait()
            for unit in range(PIECES[kind]):
                forward(kind, unit, 0, 0, 0)
            to_partner(kind, 0, 0, 0)
            if kind < 2:
                loads[kind].wait()
                if kind == 0:
                    loads[1].start()
                add(kind, me)
        elif what == "near":
            _, _, unit, r, yy, j = step
            block = block_of(kind, r, yy, j)
            wait(view(kind, block, unit), landing(kind, block, unit))
            forward(kind, unit, r, yy, j)
            arrived[kind, r, yy, j] = arrived.get((kind, r, yy, j), 0) + 1
            if arrived[kind, r, yy, j] == PIECES[kind]:
                to_partner(kind, r, yy, j)
                if kind < 2:
                    add(kind, block)
        elif what == "partner":
            _, _, r, yy, j = step
            block = block_of(kind, r, yy, j, True)
            wait(view(kind, block), landing(kind, block, 0))
            if kind < 2:
                add(kind, block)
        else:
            grad_pre[rep] = acc_g[...].astype(jnp.bfloat16)
            swap.start()
    swap.wait()
    for copy, when in sent:
        if when is None:
            copy.wait_send()
        else:
            pl.when(when)(copy.wait_send)


SLOTS = 4


def product_kernel(grad_ref, act_ref, out_hbm, tiles, sems):
    reps, zero, group, width = act_ref.shape
    tokens = reps * group
    rows = jnp.concatenate([grad_ref[r] for r in range(reps)], axis=1)
    copies = []
    for i in range(zero):
        slot = i % SLOTS
        if i >= SLOTS:
            copies[i - SLOTS].wait()
        block = jnp.concatenate([act_ref[r, i] for r in range(reps)], axis=0)
        summed = jnp.dot(rows, block, preferred_element_type=jnp.float32)
        if tokens & (tokens - 1):
            tiles[slot] = summed / jnp.float32(tokens)
        else:
            tiles[slot] = summed * jnp.float32(1 / tokens)
        copy = pltpu.make_async_copy(
            tiles.at[slot], out_hbm.at[:, pl.ds(i * width, width)], sems.at[slot]
        )
        copy.start()
        copies.append(copy)
    for copy in copies[-SLOTS:]:
        copy.wait()


def fused(acts, grads_out, act_inverse, grad_inverse):
    group, width = acts.shape
    zero = lax.axis_size("zero")
    reps = lax.axis_size("rep")
    rows, cols = act_inverse.shape
    outer = zero // 4
    bf16, dma = jnp.bfloat16, pltpu.SemaphoreType.DMA
    vmem = pl.BlockSpec(memory_space=pltpu.VMEM)
    hbm = pl.BlockSpec(memory_space=pltpu.HBM)
    order = schedule(outer)
    act_pre, grad_pre = pl.pallas_call(
        functools.partial(gather_kernel, outer, order),
        out_shape=(
            jax.ShapeDtypeStruct((reps * zero, group, width), bf16),
            jax.ShapeDtypeStruct((reps, width, group), bf16),
        ),
        in_specs=[hbm, hbm, hbm, hbm],
        out_specs=(vmem, vmem),
        scratch_shapes=[
            pltpu.VMEM((rows, cols), bf16),
            pltpu.VMEM((rows, cols), bf16),
            pltpu.VMEM((2, zero, group, width), bf16),
            pltpu.VMEM((group, width), jnp.float32),
            pltpu.VMEM((width, group), jnp.float32),
            dma((2,)),
            dma((sends_of(order),)),
            dma((2, zero, max(PIECES[:2]))),
            dma((reps * zero, PIECES[2])),
            dma,
            dma((3,)),
        ],
        compiler_params=pltpu.CompilerParams(
            collective_id=0, has_side_effects=True, vmem_limit_bytes=KERNEL_VMEM
        ),
    )(acts, grads_out, act_inverse, grad_inverse)
    return pl.pallas_call(
        product_kernel,
        out_shape=jax.ShapeDtypeStruct((rows, cols), jnp.float32),
        in_specs=[vmem, vmem],
        out_specs=hbm,
        scratch_shapes=[pltpu.VMEM((SLOTS, rows, width), jnp.float32), dma((SLOTS,))],
        compiler_params=pltpu.CompilerParams(vmem_limit_bytes=32 * 1024 * 1024),
    )(grad_pre, act_pre.reshape(reps, zero, group, width))


def on_device(acts, grads_out, act_inverse, grad_inverse):
    whole = acts.shape[1] % 128 == 0 and acts.shape[0] % 128 == 0
    if whole and lax.axis_size("rep") == 2 and lax.axis_size("zero") // 4 in ORDERS and lax.axis_size("zero") % 4 == 0:
        return fused(acts, grads_out, act_inverse, grad_inverse)
    return gathered(acts, grads_out, act_inverse, grad_inverse)


def solution(mesh):
    return jax.shard_map(
        on_device,
        mesh=mesh,
        in_specs=(P("rep", "zero"), P("rep", "zero"), P("zero", None), P("zero", None)),
        out_specs=P("zero", None),
        check_vma=False,
    )
```

```python
import functools

import jax
import jax.numpy as jnp
from jax import lax
from jax.experimental import pallas as pl
from jax.experimental.pallas import tpu as pltpu
from jax.sharding import PartitionSpec as P

NT = (((1,), (1,)), ((), ()))


def gathered(acts, grads_out, act_inverse, grad_inverse):
    group = acts.shape[0]
    total_tokens = group * lax.axis_size("rep")
    both = lax.all_gather(jnp.concatenate([acts, grads_out], 0), "zero", axis=1, tiled=True)
    act_own = lax.dot_general(
        both[:group], act_inverse, NT, preferred_element_type=jnp.float32
    ).astype(jnp.bfloat16)
    act_pre = lax.all_gather(act_own, ("rep", "zero"), axis=0)
    grad_own = lax.dot_general(
        both[group:], grad_inverse, NT, preferred_element_type=jnp.float32
    ).astype(jnp.bfloat16)
    grad_pre = lax.all_gather(grad_own, "rep", axis=0, tiled=True)
    zero = lax.axis_size("zero")
    act_pre = act_pre.reshape(-1, zero, group, act_own.shape[1]).transpose(0, 2, 1, 3)
    act_pre = act_pre.reshape(total_tokens, -1)
    summed = lax.dot_general(
        grad_pre, act_pre, (((0,), (0,)), ((), ())), preferred_element_type=jnp.float32
    )
    return summed / jnp.float32(total_tokens)


MESH = pl.DeviceIdType.MESH

PIECES = (4, 2, 2)
SWAPPED = (0, 0, 1)
ROUND_Y, ROUND_Z = 2, 1
HOLD = 8
KERNEL_VMEM = 46137344

ORDERS = {4: [('own', 0), ('near', 0, 0, 0, 0, 1), ('near', 0, 0, 0, 0, 2), ('near', 0, 0, 0, 1, 0), ('near', 0, 1, 0, 0, 2), ('near', 0, 1, 0, 1, 0), ('near', 0, 3, 0, 0, 1), ('near', 0, 1, 0, 0, 1), ('near', 0, 0, 0, 1, 1), ('near', 0, 3, 0, 1, 0), ('near', 0, 2, 0, 0, 2), ('near', 0, 3, 0, 0, 2), ('near', 0, 2, 0, 0, 1), ('partner', 0, 0, 0, 0), ('near', 0, 0, 0, 0, 3), ('near', 0, 1, 0, 0, 3), ('near', 0, 2, 0, 0, 3), ('near', 0, 3, 0, 0, 3), ('near', 0, 1, 0, 1, 2), ('near', 0, 1, 0, 1, 1), ('near', 0, 2, 0, 1, 0), ('near', 0, 3, 0, 1, 2), ('partner', 0, 0, 0, 2), ('near', 0, 3, 0, 1, 1), ('near', 0, 2, 0, 1, 2), ('near', 0, 0, 0, 1, 2), ('own', 1), ('near', 0, 2, 0, 1, 1), ('partner', 0, 0, 0, 1), ('partner', 0, 0, 0, 3), ('partner', 0, 0, 1, 2), ('near', 0, 1, 0, 1, 3), ('partner', 0, 0, 1, 1), ('near', 0, 2, 0, 1, 3), ('near', 0, 0, 0, 1, 3), ('near', 0, 3, 0, 1, 3), ('partner', 0, 0, 1, 0), ('near', 1, 0, 0, 0, 2), ('partner', 0, 0, 1, 3), ('own', 2), ('near', 1, 1, 0, 1, 0), ('near', 2, 0, 0, 0, 2), ('near', 1, 0, 0, 1, 0), ('near', 1, 0, 0, 0, 1), ('near', 2, 1, 0, 0, 2), ('near', 2, 1, 0, 1, 0), ('near', 1, 1, 0, 0, 1), ('partner', 1, 0, 0, 0), ('near', 2, 0, 0, 0, 1), ('near', 2, 1, 0, 0, 1), ('near', 2, 0, 0, 1, 2), ('near', 1, 1, 0, 0, 2), ('near', 2, 1, 0, 1, 2), ('near', 1, 0, 0, 0, 3), ('near', 2, 1, 0, 1, 1), ('near', 2, 0, 0, 1, 1), ('near', 1, 1, 0, 1, 1), ('near', 1, 0, 0, 1, 1), ('near', 1, 1, 0, 0, 3), ('near', 2, 0, 0, 0, 3), ('near', 1, 1, 0, 1, 2), ('partner', 1, 0, 0, 2), ('near', 1, 0, 0, 1, 2), ('partner', 1, 0, 1, 1), ('near', 2, 1, 0, 1, 3), ('near', 1, 1, 0, 1, 3), ('near', 2, 1, 1, 0, 1), ('near', 1, 0, 0, 1, 3), ('partner', 1, 0, 1, 0), ('near', 2, 1, 0, 0, 3), ('near', 2, 0, 1, 0, 0), ('near', 2, 1, 1, 0, 0), ('partner', 1, 0, 0, 1), ('partner', 1, 0, 1, 2), ('near', 2, 0, 1, 1, 1), ('partner', 1, 0, 0, 3), ('near', 2, 0, 0, 1, 3), ('near', 2, 0, 1, 0, 3), ('partner', 1, 0, 1, 3), ('near', 2, 0, 1, 0, 2), ('swap', 1), ('near', 2, 1, 1, 1, 3), ('near', 2, 1, 1, 1, 1), ('near', 2, 1, 1, 0, 3), ('near', 2, 0, 1, 1, 2), ('near', 2, 0, 0, 1, 0), ('near', 2, 0, 1, 0, 1), ('near', 2, 0, 1, 1, 3), ('near', 2, 0, 1, 1, 0), ('near', 2, 1, 1, 1, 0), ('near', 2, 1, 1, 0, 2), ('near', 2, 1, 1, 1, 2), ('partner', 2, 0, 0, 0), ('partner', 2, 0, 0, 1), ('partner', 2, 0, 0, 2), ('partner', 2, 0, 0, 3), ('partner', 2, 0, 1, 0), ('partner', 2, 0, 1, 1), ('partner', 2, 0, 1, 2), ('partner', 2, 0, 1, 3), ('partner', 2, 1, 0, 0), ('partner', 2, 1, 0, 1), ('partner', 2, 1, 0, 2), ('partner', 2, 1, 0, 3), ('partner', 2, 1, 1, 0), ('partner', 2, 1, 1, 1), ('partner', 2, 1, 1, 2), ('partner', 2, 1, 1, 3)]}


def schedule(outer):
    return ORDERS[outer]


def nearest_first(outer):
    rows = []
    for z in range(outer):
        others = [q for q in range(outer) if q != z]
        others.sort(key=lambda q: (abs(q - z), q if 2 * z < outer else -q))
        rows.append([z] + others)
    return rows


def hops(kind, unit, r, yy, j):
    by_y, by_z = unit < ROUND_Y, unit < ROUND_Z
    if r == 1:
        if yy == 0 and j == 0:
            return ["y"] * by_y + ["up", "down"] * by_z
        return []
    ways = []
    if kind == 2:
        if yy == 1 and j == 0:
            ways += ["x"] * (not by_y)
        elif yy == 0 and j in (1, 2) and by_z:
            ways += ["x far"] * (j == 2)
        else:
            ways += ["x"]
    late = unit >= PIECES[kind] - SWAPPED[kind]
    if yy == 0 or late:
        ways += ["up", "down"] if j == 0 else ["on"]
    if yy == 0 and (j == 0 or not late):
        ways += ["y"]
    return ways


def sends_of(order):
    count, seen = 0, {}
    for what, kind, *rest in order:
        if what == "own":
            count += 1 + sum(len(hops(kind, unit, 0, 0, 0)) for unit in range(PIECES[kind]))
        elif what == "near":
            key = (kind, *rest[1:])
            seen[key] = seen.get(key, 0) + 1
            count += len(hops(kind, *rest)) + (seen[key] == PIECES[kind])
    return count


def gather_kernel(
    outer, order, acts, grads, a_hbm, g_hbm, pre, grad_pre,
    a_rows, g_rows, held, acc_a, acc_g,
    w_sem, send_sem, recv, recv_pre, x_recv, own_sem,
):
    group, width = acts.shape
    zero = outer * 4
    rep = lax.axis_index("rep")
    me = lax.axis_index("zero")
    z, y, c = me // 4, (me // 2) % 2, me % 2

    own = [
        pltpu.make_async_copy(acts, held.at[0, me], own_sem.at[0]),
        pltpu.make_async_copy(grads, held.at[1, me], own_sem.at[1]),
    ]
    loads = [
        pltpu.make_async_copy(a_hbm, a_rows, w_sem.at[0]),
        pltpu.make_async_copy(g_hbm, g_rows, w_sem.at[1]),
    ]
    own[0].start()
    own[1].start()

    x_peer = (1 - rep, me)
    y_peer = (rep, z * 4 + (1 - y) * 2 + c)
    c_peer = (rep, z * 4 + y * 2 + 1 - c)
    has_up, has_down = z < outer - 1, z > 0

    def z_peer(to):
        return (rep, to * 4 + y * 2 + c)

    barrier = pltpu.get_barrier_semaphore()

    def greet(peer):
        pl.semaphore_signal(barrier, inc=1, device_id=peer, device_id_type=MESH)

    for peer in (x_peer, y_peer, c_peer):
        greet(peer)
    pl.when(has_up)(lambda: greet(z_peer(z + 1)))
    pl.when(has_down)(lambda: greet(z_peer(z - 1)))
    pl.semaphore_wait(barrier, 3 + has_up.astype(jnp.int32) + has_down.astype(jnp.int32))

    table = nearest_first(outer)
    at_z = []
    for j in range(outer):
        value = jnp.int32(table[0][j])
        for q in range(1, outer):
            value = jnp.where(z == q, table[q][j], value)
        at_z.append(value)

    def block_of(kind, r, yy, j, other=False):
        cc = 1 - c if other else c
        block = at_z[j] * 4 + ((y + yy) % 2) * 2 + cc
        if kind == 2:
            block += ((rep + r) % 2) * zero
        return block

    def view(kind, block, unit=None):
        ref = pre.at[block] if kind == 2 else held.at[kind, block]
        if unit is None:
            return ref
        rows = group // PIECES[kind]
        return ref.at[pl.ds(unit * rows, rows)]

    def landing(kind, block, unit):
        return recv_pre.at[block, unit] if kind == 2 else recv.at[kind, block, unit]

    sent = []

    def send(ref, peer, arrival, when=None):
        copy = pltpu.make_async_remote_copy(
            src_ref=ref, dst_ref=ref,
            send_sem=send_sem.at[len(sent)], recv_sem=arrival,
            device_id=peer, device_id_type=MESH,
        )
        sent.append((copy, when))
        if when is None:
            copy.start()
        else:
            pl.when(when)(copy.start)

    def forward(kind, unit, r, yy, j):
        block = block_of(kind, r, yy, j)
        ref, arrival = view(kind, block, unit), landing(kind, block, unit)
        onward = jnp.where(at_z[j] < z, z + 1, z - 1)
        ways = {
            "x": (x_peer, None),
            "x far": (x_peer, jnp.abs(at_z[j] - z) > 1),
            "y": (y_peer, None),
            "up": (z_peer(z + 1), has_up),
            "down": (z_peer(z - 1), has_down),
            "on": (z_peer(onward), (onward >= 0) & (onward < outer)),
        }
        for way in hops(kind, unit, r, yy, j):
            peer, when = ways[way]
            send(ref, peer, arrival, when)

    def to_partner(kind, r, yy, j):
        block = block_of(kind, r, yy, j)
        send(view(kind, block), c_peer, landing(kind, block, 0))

    begun = [False, False]
    waiting = [[], []]

    def catch_up(kind, count):
        if waiting[kind] and not begun[kind]:
            loads[kind].wait()
            if kind == 0:
                loads[1].start()
        for block in waiting[kind][:count]:
            add(kind, block)
        del waiting[kind][:count]

    def add(kind, block):
        value = held[kind, block]
        columns = pl.ds(pl.multiple_of(block * width, width), width)
        if kind == 0:
            acc, term = acc_a, lax.dot_general(
                value, a_rows[:, columns], NT, preferred_element_type=jnp.float32
            )
        else:
            acc, term = acc_g, lax.dot_general(
                g_rows[:, columns], value, NT, preferred_element_type=jnp.float32
            )
        if begun[kind]:
            acc[...] += term
        else:
            acc[...] = term
            begun[kind] = True

    def wait(ref, arrival):
        pltpu.make_async_copy(ref, ref, arrival).wait()

    mine = rep * zero + me
    arrived = {}
    swap = pltpu.make_async_remote_copy(
        src_ref=grad_pre.at[rep], dst_ref=grad_pre.at[rep],
        send_sem=own_sem.at[2], recv_sem=x_recv,
        device_id=x_peer, device_id_type=MESH,
    )
    for place, step in enumerate(order):
        what, kind = step[0], step[1]
        if place > HOLD:
            catch_up(0, 2)
        if place > HOLD and not waiting[0]:
            catch_up(1, 1)
        if what == "own":
            if kind == 2:
                catch_up(0, len(waiting[0]))
                pre[mine] = acc_a[...].astype(jnp.bfloat16)
            else:
                own[kind].wait()
            for unit in range(PIECES[kind]):
                forward(kind, unit, 0, 0, 0)
            to_partner(kind, 0, 0, 0)
            if kind < 2:
                waiting[kind].append(me)
            if kind == 0:
                loads[0].start()
        elif what == "near":
            _, _, unit, r, yy, j = step
            block = block_of(kind, r, yy, j)
            wait(view(kind, block, unit), landing(kind, block, unit))
            forward(kind, unit, r, yy, j)
            arrived[kind, r, yy, j] = arrived.get((kind, r, yy, j), 0) + 1
            if arrived[kind, r, yy, j] == PIECES[kind]:
                to_partner(kind, r, yy, j)
                if kind < 2:
                    waiting[kind].append(block)
        elif what == "partner":
            _, _, r, yy, j = step
            block = block_of(kind, r, yy, j, True)
            wait(view(kind, block), landing(kind, block, 0))
            if kind < 2:
                waiting[kind].append(block)
        else:
            catch_up(1, len(waiting[1]))
            grad_pre[rep] = acc_g[...].astype(jnp.bfloat16)
            swap.start()
    swap.wait()
    for copy, when in sent:
        if when is None:
            copy.wait_send()
        else:
            pl.when(when)(copy.wait_send)


SLOTS = 4


def product_kernel(grad_ref, act_ref, out_hbm, tiles, sems):
    reps, zero, group, width = act_ref.shape
    tokens = reps * group
    rows = jnp.concatenate([grad_ref[r] for r in range(reps)], axis=1)
    copies = []
    for i in range(zero):
        slot = i % SLOTS
        if i >= SLOTS:
            copies[i - SLOTS].wait()
        block = jnp.concatenate([act_ref[r, i] for r in range(reps)], axis=0)
        summed = jnp.dot(rows, block, preferred_element_type=jnp.float32)
        if tokens & (tokens - 1):
            tiles[slot] = summed / jnp.float32(tokens)
        else:
            tiles[slot] = summed * jnp.float32(1 / tokens)
        copy = pltpu.make_async_copy(
            tiles.at[slot], out_hbm.at[:, pl.ds(i * width, width)], sems.at[slot]
        )
        copy.start()
        copies.append(copy)
    for copy in copies[-SLOTS:]:
        copy.wait()


def fused(acts, grads_out, act_inverse, grad_inverse):
    group, width = acts.shape
    zero = lax.axis_size("zero")
    reps = lax.axis_size("rep")
    rows, cols = act_inverse.shape
    outer = zero // 4
    bf16, dma = jnp.bfloat16, pltpu.SemaphoreType.DMA
    vmem = pl.BlockSpec(memory_space=pltpu.VMEM)
    hbm = pl.BlockSpec(memory_space=pltpu.HBM)
    order = schedule(outer)
    act_pre, grad_pre = pl.pallas_call(
        functools.partial(gather_kernel, outer, order),
        out_shape=(
            jax.ShapeDtypeStruct((reps * zero, group, width), bf16),
            jax.ShapeDtypeStruct((reps, width, group), bf16),
        ),
        in_specs=[hbm, hbm, hbm, hbm],
        out_specs=(vmem, vmem),
        scratch_shapes=[
            pltpu.VMEM((rows, cols), bf16),
            pltpu.VMEM((rows, cols), bf16),
            pltpu.VMEM((2, zero, group, width), bf16),
            pltpu.VMEM((group, width), jnp.float32),
            pltpu.VMEM((width, group), jnp.float32),
            dma((2,)),
            dma((sends_of(order),)),
            dma((2, zero, max(PIECES[:2]))),
            dma((reps * zero, PIECES[2])),
            dma,
            dma((3,)),
        ],
        compiler_params=pltpu.CompilerParams(
            collective_id=0, has_side_effects=True, vmem_limit_bytes=KERNEL_VMEM
        ),
    )(*(pltpu.with_memory_space_constraint(a, pltpu.HBM) for a in (acts, grads_out, act_inverse, grad_inverse)))
    return pl.pallas_call(
        product_kernel,
        out_shape=jax.ShapeDtypeStruct((rows, cols), jnp.float32),
        in_specs=[vmem, vmem],
        out_specs=hbm,
        scratch_shapes=[pltpu.VMEM((SLOTS, rows, width), jnp.float32), dma((SLOTS,))],
        compiler_params=pltpu.CompilerParams(vmem_limit_bytes=32 * 1024 * 1024),
    )(grad_pre, act_pre.reshape(reps, zero, group, width))


def on_device(acts, grads_out, act_inverse, grad_inverse):
    whole = acts.shape[1] % 128 == 0 and acts.shape[0] % 128 == 0
    if whole and lax.axis_size("rep") == 2 and lax.axis_size("zero") // 4 in ORDERS and lax.axis_size("zero") % 4 == 0:
        return fused(acts, grads_out, act_inverse, grad_inverse)
    return gathered(acts, grads_out, act_inverse, grad_inverse)


def solution(mesh):
    return jax.shard_map(
        on_device,
        mesh=mesh,
        in_specs=(P("rep", "zero"), P("rep", "zero"), P("zero", None), P("zero", None)),
        out_specs=P("zero", None),
        check_vma=False,
    )
```

```python
import functools

import jax
import jax.numpy as jnp
from jax import lax
from jax.experimental import pallas as pl
from jax.experimental.pallas import tpu as pltpu
from jax.sharding import PartitionSpec as P

NT = (((1,), (1,)), ((), ()))


def gathered(acts, grads_out, act_inverse, grad_inverse):
    group = acts.shape[0]
    total_tokens = group * lax.axis_size("rep")
    both = lax.all_gather(jnp.concatenate([acts, grads_out], 0), "zero", axis=1, tiled=True)
    act_own = lax.dot_general(
        both[:group], act_inverse, NT, preferred_element_type=jnp.float32
    ).astype(jnp.bfloat16)
    act_pre = lax.all_gather(act_own, ("rep", "zero"), axis=0)
    grad_own = lax.dot_general(
        both[group:], grad_inverse, NT, preferred_element_type=jnp.float32
    ).astype(jnp.bfloat16)
    grad_pre = lax.all_gather(grad_own, "rep", axis=0, tiled=True)
    zero = lax.axis_size("zero")
    act_pre = act_pre.reshape(-1, zero, group, act_own.shape[1]).transpose(0, 2, 1, 3)
    act_pre = act_pre.reshape(total_tokens, -1)
    summed = lax.dot_general(
        grad_pre, act_pre, (((0,), (0,)), ((), ())), preferred_element_type=jnp.float32
    )
    return summed / jnp.float32(total_tokens)


MESH = pl.DeviceIdType.MESH

PIECES = (4, 2, 2)
SWAPPED = (0, 0, 1)
ROUND_Y, ROUND_Z = 2, 1
HOLD = 8
PARTS = (2, 1, 1)
KERNEL_VMEM = 46137344

ORDERS = {4: [('own', 0), ('near', 0, 0, 0, 0, 1), ('near', 0, 1, 0, 0, 1), ('near', 0, 1, 0, 1, 0), ('near', 0, 0, 0, 1, 0), ('near', 0, 2, 0, 0, 1), ('near', 0, 1, 0, 0, 2), ('near', 0, 0, 0, 0, 2), ('near', 0, 3, 0, 0, 1), ('near', 0, 0, 0, 1, 1), ('near', 0, 0, 0, 0, 3), ('near', 0, 1, 0, 0, 3), ('partner', 0, 0, 0, 0, 1), ('near', 0, 1, 0, 1, 1), ('near', 0, 3, 0, 0, 2), ('partner', 0, 0, 0, 1, 0), ('near', 0, 1, 0, 1, 2), ('near', 0, 3, 0, 1, 0), ('near', 0, 2, 0, 0, 2), ('near', 0, 2, 0, 0, 3), ('partner', 0, 1, 0, 0, 1), ('partner', 0, 0, 0, 0, 2), ('near', 0, 3, 0, 0, 3), ('own', 1), ('near', 0, 2, 0, 1, 0), ('near', 0, 2, 0, 1, 1), ('near', 0, 3, 0, 1, 1), ('partner', 0, 1, 0, 0, 0), ('partner', 0, 0, 0, 1, 1), ('near', 0, 0, 0, 1, 3), ('partner', 0, 0, 0, 0, 3), ('near', 0, 0, 0, 1, 2), ('partner', 0, 0, 0, 0, 0), ('near', 0, 1, 0, 1, 3), ('partner', 0, 1, 0, 0, 3), ('partner', 0, 0, 0, 1, 2), ('partner', 0, 1, 0, 0, 2), ('partner', 0, 0, 0, 1, 3), ('near', 0, 3, 0, 1, 2), ('partner', 0, 1, 0, 1, 0), ('own', 2, 0), ('near', 0, 2, 0, 1, 2), ('partner', 0, 1, 0, 1, 1), ('near', 0, 3, 0, 1, 3), ('near', 0, 2, 0, 1, 3), ('partner', 0, 1, 0, 1, 2), ('near', 1, 1, 0, 0, 2), ('partner', 0, 1, 0, 1, 3), ('own', 2, 1), ('near', 2, 0, 0, 0, 2), ('near', 1, 0, 0, 1, 0), ('near', 1, 1, 0, 0, 1), ('near', 2, 1, 0, 0, 2), ('near', 2, 0, 0, 0, 1), ('near', 1, 1, 0, 0, 3), ('near', 2, 1, 0, 1, 0), ('near', 2, 1, 0, 0, 1), ('near', 2, 0, 0, 1, 2), ('near', 1, 1, 0, 1, 0), ('near', 1, 0, 0, 0, 1), ('near', 2, 0, 0, 0, 3), ('near', 2, 1, 0, 1, 2), ('near', 2, 0, 0, 1, 1), ('near', 1, 0, 0, 0, 2), ('near', 2, 1, 0, 1, 1), ('partner', 1, 0, 0, 0, 1), ('near', 1, 1, 0, 1, 2), ('near', 1, 0, 0, 0, 3), ('near', 1, 0, 0, 1, 1), ('near', 2, 0, 1, 1, 2), ('partner', 1, 0, 0, 0, 0), ('partner', 1, 0, 0, 0, 2), ('partner', 1, 0, 0, 1, 0), ('near', 2, 1, 0, 0, 3), ('near', 1, 1, 0, 1, 3), ('near', 1, 1, 0, 1, 1), ('near', 2, 1, 0, 1, 3), ('near', 1, 0, 0, 1, 2), ('near', 2, 0, 1, 0, 0), ('near', 2, 0, 1, 1, 1), ('near', 1, 0, 0, 1, 3), ('near', 2, 1, 1, 1, 1), ('near', 2, 1, 1, 0, 0), ('near', 2, 1, 1, 0, 2), ('near', 2, 1, 1, 1, 2), ('near', 2, 0, 0, 1, 3), ('partner', 1, 0, 0, 1, 1), ('partner', 1, 0, 0, 1, 2), ('partner', 1, 0, 0, 0, 3), ('partner', 1, 0, 0, 1, 3), ('swap', 1), ('near', 2, 1, 1, 0, 3), ('near', 2, 1, 1, 1, 3), ('near', 2, 0, 1, 0, 2), ('near', 2, 0, 1, 1, 0), ('near', 2, 0, 1, 0, 3), ('near', 2, 0, 0, 1, 0), ('near', 2, 0, 1, 1, 3), ('near', 2, 0, 1, 0, 1), ('near', 2, 1, 1, 1, 0), ('near', 2, 1, 1, 0, 1), ('partner', 2, 0, 0, 0, 0), ('partner', 2, 0, 0, 0, 1), ('partner', 2, 0, 0, 0, 2), ('partner', 2, 0, 0, 0, 3), ('partner', 2, 0, 0, 1, 0), ('partner', 2, 0, 0, 1, 1), ('partner', 2, 0, 0, 1, 2), ('partner', 2, 0, 0, 1, 3), ('partner', 2, 0, 1, 0, 0), ('partner', 2, 0, 1, 0, 1), ('partner', 2, 0, 1, 0, 2), ('partner', 2, 0, 1, 0, 3), ('partner', 2, 0, 1, 1, 0), ('partner', 2, 0, 1, 1, 1), ('partner', 2, 0, 1, 1, 2), ('partner', 2, 0, 1, 1, 3)]}


def schedule(outer):
    return ORDERS[outer]


def nearest_first(outer):
    rows = []
    for z in range(outer):
        others = [q for q in range(outer) if q != z]
        others.sort(key=lambda q: (abs(q - z), q if 2 * z < outer else -q))
        rows.append([z] + others)
    return rows


def hops(kind, unit, r, yy, j):
    by_y, by_z = unit < ROUND_Y, unit < ROUND_Z
    if r == 1:
        if yy == 0 and j == 0:
            return ["y"] * by_y + ["up", "down"] * by_z
        return []
    ways = []
    if kind == 2:
        if yy == 1 and j == 0:
            ways += ["x"] * (not by_y)
        elif yy == 0 and j in (1, 2) and by_z:
            ways += ["x far"] * (j == 2)
        else:
            ways += ["x"]
    late = unit >= PIECES[kind] - SWAPPED[kind]
    if yy == 0 or late:
        ways += ["up", "down"] if j == 0 else ["on"]
    if yy == 0 and (j == 0 or not late):
        ways += ["y"]
    return ways


def part_of(kind, unit):
    return unit * PARTS[kind] // PIECES[kind]


def units_of(kind, part=None):
    if part is None:
        return range(PIECES[kind])
    return range(part * PIECES[kind] // PARTS[0], (part + 1) * PIECES[kind] // PARTS[0])


def sends_of(order):
    count, seen = 0, {}
    for what, kind, *rest in order:
        if what == "own":
            units = units_of(kind, *rest)
            count += sum(len(hops(kind, unit, 0, 0, 0)) for unit in units)
            count += PARTS[kind] if kind == 0 else PIECES[kind] - 1 in units
        elif what == "near":
            key = (kind, part_of(kind, rest[0]), *rest[1:])
            seen[key] = seen.get(key, 0) + 1
            count += len(hops(kind, *rest)) + (seen[key] == PIECES[kind] // PARTS[kind])
    return count


def gather_kernel(
    outer, order, acts, grads, a_hbm, g_hbm, pre, grad_pre,
    a_rows, g_rows, held, acc_a, acc_g,
    w_sem, send_sem, recv, recv_pre, x_recv, own_sem,
):
    group, width = acts.shape
    zero = outer * 4
    rep = lax.axis_index("rep")
    me = lax.axis_index("zero")
    z, y, c = me // 4, (me // 2) % 2, me % 2

    own = [
        pltpu.make_async_copy(acts, held.at[0, me], own_sem.at[0]),
        pltpu.make_async_copy(grads, held.at[1, me], own_sem.at[1]),
    ]
    loads = [
        pltpu.make_async_copy(a_hbm, a_rows, w_sem.at[0]),
        pltpu.make_async_copy(g_hbm, g_rows, w_sem.at[1]),
    ]
    own[0].start()
    own[1].start()

    x_peer = (1 - rep, me)
    y_peer = (rep, z * 4 + (1 - y) * 2 + c)
    c_peer = (rep, z * 4 + y * 2 + 1 - c)
    has_up, has_down = z < outer - 1, z > 0

    def z_peer(to):
        return (rep, to * 4 + y * 2 + c)

    barrier = pltpu.get_barrier_semaphore()

    def greet(peer):
        pl.semaphore_signal(barrier, inc=1, device_id=peer, device_id_type=MESH)

    for peer in (x_peer, y_peer, c_peer):
        greet(peer)
    pl.when(has_up)(lambda: greet(z_peer(z + 1)))
    pl.when(has_down)(lambda: greet(z_peer(z - 1)))
    pl.semaphore_wait(barrier, 3 + has_up.astype(jnp.int32) + has_down.astype(jnp.int32))

    table = nearest_first(outer)
    at_z = []
    for j in range(outer):
        value = jnp.int32(table[0][j])
        for q in range(1, outer):
            value = jnp.where(z == q, table[q][j], value)
        at_z.append(value)

    def block_of(kind, r, yy, j, other=False):
        cc = 1 - c if other else c
        block = at_z[j] * 4 + ((y + yy) % 2) * 2 + cc
        if kind == 2:
            block += ((rep + r) % 2) * zero
        return block

    def view(kind, block, unit=None):
        ref = pre.at[block] if kind == 2 else held.at[kind, block]
        if unit is None:
            return ref
        rows = group // PIECES[kind]
        return ref.at[pl.ds(unit * rows, rows)]

    def part_view(kind, block, part):
        if PARTS[kind] == 1:
            return view(kind, block)
        rows = group // PARTS[kind]
        return held.at[kind, block, pl.ds(part * rows, rows)]

    def landing(kind, block, unit):
        return recv_pre.at[block, unit] if kind == 2 else recv.at[kind, block, unit]

    sent = []

    def send(ref, peer, arrival, when=None):
        copy = pltpu.make_async_remote_copy(
            src_ref=ref, dst_ref=ref,
            send_sem=send_sem.at[len(sent)], recv_sem=arrival,
            device_id=peer, device_id_type=MESH,
        )
        sent.append((copy, when))
        if when is None:
            copy.start()
        else:
            pl.when(when)(copy.start)

    def forward(kind, unit, r, yy, j):
        block = block_of(kind, r, yy, j)
        ref, arrival = view(kind, block, unit), landing(kind, block, unit)
        onward = jnp.where(at_z[j] < z, z + 1, z - 1)
        ways = {
            "x": (x_peer, None),
            "x far": (x_peer, jnp.abs(at_z[j] - z) > 1),
            "y": (y_peer, None),
            "up": (z_peer(z + 1), has_up),
            "down": (z_peer(z - 1), has_down),
            "on": (z_peer(onward), (onward >= 0) & (onward < outer)),
        }
        for way in hops(kind, unit, r, yy, j):
            peer, when = ways[way]
            send(ref, peer, arrival, when)

    def to_partner(kind, part, r, yy, j):
        block = block_of(kind, r, yy, j)
        send(part_view(kind, block, part), c_peer, landing(kind, block, part))

    begun = [False] * 3
    waiting = [[], [], []]

    def catch_up(lot, count):
        kind = 1 if lot == PARTS[0] else 0
        if waiting[lot] and not any(begun[:2] if kind == 0 else begun[2:]):
            loads[kind].wait()
            if kind == 0:
                loads[1].start()
        for block in waiting[lot][:count]:
            add(lot, kind, block)
        del waiting[lot][:count]

    def add(lot, kind, block):
        columns = pl.ds(pl.multiple_of(block * width, width), width)
        if kind == 0:
            rows = group // PARTS[0]
            span = pl.ds(lot * rows, rows)
            acc = acc_a.at[span]
            term = lax.dot_general(
                held[0, block, span], a_rows[:, columns], NT, preferred_element_type=jnp.float32
            )
        else:
            acc = acc_g
            term = lax.dot_general(
                g_rows[:, columns], held[1, block], NT, preferred_element_type=jnp.float32
            )
        if begun[lot]:
            acc[...] += term
        else:
            acc[...] = term
            begun[lot] = True

    def wait(ref, arrival):
        pltpu.make_async_copy(ref, ref, arrival).wait()

    mine = rep * zero + me
    arrived = {}
    swap = pltpu.make_async_remote_copy(
        src_ref=grad_pre.at[rep], dst_ref=grad_pre.at[rep],
        send_sem=own_sem.at[2], recv_sem=x_recv,
        device_id=x_peer, device_id_type=MESH,
    )
    grad_lot = PARTS[0]
    for place, step in enumerate(order):
        what, kind = step[0], step[1]
        if place > HOLD:
            lot = next((q for q in range(grad_lot + 1) if waiting[q]), grad_lot)
            catch_up(lot, 2 if lot < grad_lot else 1)
        if what == "own":
            if kind == 2:
                part = step[2]
                catch_up(part, len(waiting[part]))
                rows = group // PARTS[0]
                span = pl.ds(part * rows, rows)
                pre[mine, span] = acc_a[span].astype(jnp.bfloat16)
            else:
                own[kind].wait()
            units = units_of(*step[1:])
            for unit in units:
                forward(kind, unit, 0, 0, 0)
            if kind < 2 or PIECES[kind] - 1 in units:
                for part in range(PARTS[kind]):
                    to_partner(kind, part, 0, 0, 0)
            if kind == 0:
                loads[0].start()
                for part in range(PARTS[0]):
                    waiting[part].append(me)
            elif kind == 1:
                waiting[grad_lot].append(me)
        elif what == "near":
            _, _, unit, r, yy, j = step
            block = block_of(kind, r, yy, j)
            wait(view(kind, block, unit), landing(kind, block, unit))
            forward(kind, unit, r, yy, j)
            part = part_of(kind, unit)
            key = (kind, part, r, yy, j)
            arrived[key] = arrived.get(key, 0) + 1
            if arrived[key] == PIECES[kind] // PARTS[kind]:
                to_partner(kind, part, r, yy, j)
                if kind < 2:
                    waiting[part if kind == 0 else grad_lot].append(block)
        elif what == "partner":
            _, _, part, r, yy, j = step
            block = block_of(kind, r, yy, j, True)
            wait(part_view(kind, block, part), landing(kind, block, part))
            if kind < 2:
                waiting[part if kind == 0 else grad_lot].append(block)
        else:
            catch_up(grad_lot, len(waiting[grad_lot]))
            grad_pre[rep] = acc_g[...].astype(jnp.bfloat16)
            swap.start()
    swap.wait()
    for copy, when in sent:
        if when is None:
            copy.wait_send()
        else:
            pl.when(when)(copy.wait_send)


SLOTS = 4


def product_kernel(grad_ref, act_ref, out_hbm, tiles, sems):
    reps, zero, group, width = act_ref.shape
    tokens = reps * group
    rows = jnp.concatenate([grad_ref[r] for r in range(reps)], axis=1)
    copies = []
    for i in range(zero):
        slot = i % SLOTS
        if i >= SLOTS:
            copies[i - SLOTS].wait()
        block = jnp.concatenate([act_ref[r, i] for r in range(reps)], axis=0)
        summed = jnp.dot(rows, block, preferred_element_type=jnp.float32)
        if tokens & (tokens - 1):
            tiles[slot] = summed / jnp.float32(tokens)
        else:
            tiles[slot] = summed * jnp.float32(1 / tokens)
        copy = pltpu.make_async_copy(
            tiles.at[slot], out_hbm.at[:, pl.ds(i * width, width)], sems.at[slot]
        )
        copy.start()
        copies.append(copy)
    for copy in copies[-SLOTS:]:
        copy.wait()


def fused(acts, grads_out, act_inverse, grad_inverse):
    group, width = acts.shape
    zero = lax.axis_size("zero")
    reps = lax.axis_size("rep")
    rows, cols = act_inverse.shape
    outer = zero // 4
    bf16, dma = jnp.bfloat16, pltpu.SemaphoreType.DMA
    vmem = pl.BlockSpec(memory_space=pltpu.VMEM)
    hbm = pl.BlockSpec(memory_space=pltpu.HBM)
    order = schedule(outer)
    act_pre, grad_pre = pl.pallas_call(
        functools.partial(gather_kernel, outer, order),
        out_shape=(
            jax.ShapeDtypeStruct((reps * zero, group, width), bf16),
            jax.ShapeDtypeStruct((reps, width, group), bf16),
        ),
        in_specs=[hbm, hbm, hbm, hbm],
        out_specs=(vmem, vmem),
        scratch_shapes=[
            pltpu.VMEM((rows, cols), bf16),
            pltpu.VMEM((rows, cols), bf16),
            pltpu.VMEM((2, zero, group, width), bf16),
            pltpu.VMEM((group, width), jnp.float32),
            pltpu.VMEM((width, group), jnp.float32),
            dma((2,)),
            dma((sends_of(order),)),
            dma((2, zero, max(PIECES[:2]))),
            dma((reps * zero, PIECES[2])),
            dma,
            dma((3,)),
        ],
        compiler_params=pltpu.CompilerParams(
            collective_id=0, has_side_effects=True, vmem_limit_bytes=KERNEL_VMEM
        ),
    )(*(pltpu.with_memory_space_constraint(a, pltpu.HBM) for a in (acts, grads_out, act_inverse, grad_inverse)))
    return pl.pallas_call(
        product_kernel,
        out_shape=jax.ShapeDtypeStruct((rows, cols), jnp.float32),
        in_specs=[vmem, vmem],
        out_specs=hbm,
        scratch_shapes=[pltpu.VMEM((SLOTS, rows, width), jnp.float32), dma((SLOTS,))],
        compiler_params=pltpu.CompilerParams(vmem_limit_bytes=32 * 1024 * 1024),
    )(grad_pre, act_pre.reshape(reps, zero, group, width))


def on_device(acts, grads_out, act_inverse, grad_inverse):
    whole = acts.shape[1] % 128 == 0 and acts.shape[0] % 128 == 0
    if whole and lax.axis_size("rep") == 2 and lax.axis_size("zero") // 4 in ORDERS and lax.axis_size("zero") % 4 == 0:
        return fused(acts, grads_out, act_inverse, grad_inverse)
    return gathered(acts, grads_out, act_inverse, grad_inverse)


def solution(mesh):
    return jax.shard_map(
        on_device,
        mesh=mesh,
        in_specs=(P("rep", "zero"), P("rep", "zero"), P("zero", None), P("zero", None)),
        out_specs=P("zero", None),
        check_vma=False,
    )
```

```python
import functools

import jax
import jax.numpy as jnp
from jax import lax
from jax.experimental import pallas as pl
from jax.experimental.pallas import tpu as pltpu
from jax.sharding import PartitionSpec as P

NT = (((1,), (1,)), ((), ()))


def gathered(acts, grads_out, act_inverse, grad_inverse):
    group = acts.shape[0]
    total_tokens = group * lax.axis_size("rep")
    both = lax.all_gather(jnp.concatenate([acts, grads_out], 0), "zero", axis=1, tiled=True)
    act_own = lax.dot_general(
        both[:group], act_inverse, NT, preferred_element_type=jnp.float32
    ).astype(jnp.bfloat16)
    act_pre = lax.all_gather(act_own, ("rep", "zero"), axis=0)
    grad_own = lax.dot_general(
        both[group:], grad_inverse, NT, preferred_element_type=jnp.float32
    ).astype(jnp.bfloat16)
    grad_pre = lax.all_gather(grad_own, "rep", axis=0, tiled=True)
    zero = lax.axis_size("zero")
    act_pre = act_pre.reshape(-1, zero, group, act_own.shape[1]).transpose(0, 2, 1, 3)
    act_pre = act_pre.reshape(total_tokens, -1)
    summed = lax.dot_general(
        grad_pre, act_pre, (((0,), (0,)), ((), ())), preferred_element_type=jnp.float32
    )
    return summed / jnp.float32(total_tokens)


MESH = pl.DeviceIdType.MESH

PIECES = (4, 2, 2)
SWAPPED = (0, 0, 1)
ROUND_Y, ROUND_Z = 2, 1
HOLD = 8
PARTS = (2, 1, 2)
KERNEL_VMEM = 46137344

ORDERS = {4: [('own', 0), ('near', 0, 0, 0, 0, 1), ('near', 0, 1, 0, 0, 1), ('near', 0, 1, 0, 1, 0), ('near', 0, 0, 0, 1, 0), ('near', 0, 2, 0, 0, 1), ('near', 0, 1, 0, 0, 2), ('near', 0, 0, 0, 0, 2), ('near', 0, 3, 0, 0, 1), ('near', 0, 0, 0, 1, 1), ('near', 0, 0, 0, 0, 3), ('near', 0, 1, 0, 0, 3), ('partner', 0, 0, 0, 0, 1), ('near', 0, 1, 0, 1, 1), ('near', 0, 3, 0, 0, 2), ('partner', 0, 0, 0, 1, 0), ('near', 0, 1, 0, 1, 2), ('near', 0, 3, 0, 1, 0), ('near', 0, 2, 0, 0, 2), ('near', 0, 2, 0, 0, 3), ('partner', 0, 1, 0, 0, 1), ('partner', 0, 0, 0, 0, 2), ('near', 0, 3, 0, 0, 3), ('own', 1), ('near', 0, 2, 0, 1, 0), ('near', 0, 2, 0, 1, 1), ('near', 0, 3, 0, 1, 1), ('partner', 0, 1, 0, 0, 0), ('partner', 0, 0, 0, 1, 1), ('near', 0, 0, 0, 1, 3), ('partner', 0, 0, 0, 0, 3), ('near', 0, 0, 0, 1, 2), ('partner', 0, 0, 0, 0, 0), ('near', 0, 1, 0, 1, 3), ('partner', 0, 1, 0, 0, 3), ('partner', 0, 0, 0, 1, 2), ('partner', 0, 1, 0, 0, 2), ('partner', 0, 0, 0, 1, 3), ('near', 0, 3, 0, 1, 2), ('partner', 0, 1, 0, 1, 0), ('own', 2, 0), ('near', 0, 2, 0, 1, 2), ('partner', 0, 1, 0, 1, 1), ('near', 0, 3, 0, 1, 3), ('near', 0, 2, 0, 1, 3), ('partner', 0, 1, 0, 1, 2), ('near', 1, 1, 0, 0, 2), ('partner', 0, 1, 0, 1, 3), ('own', 2, 1), ('near', 2, 0, 0, 0, 2), ('near', 1, 0, 0, 1, 0), ('near', 1, 1, 0, 0, 1), ('near', 2, 1, 0, 0, 2), ('near', 2, 0, 0, 0, 1), ('near', 1, 1, 0, 0, 3), ('near', 2, 1, 0, 1, 0), ('near', 2, 1, 0, 0, 1), ('near', 2, 0, 0, 1, 2), ('near', 1, 1, 0, 1, 0), ('near', 1, 0, 0, 0, 1), ('near', 2, 0, 0, 0, 3), ('near', 2, 1, 0, 1, 2), ('near', 2, 0, 0, 1, 1), ('near', 1, 0, 0, 0, 2), ('near', 2, 1, 0, 1, 1), ('partner', 1, 0, 0, 0, 1), ('near', 1, 1, 0, 1, 2), ('near', 1, 0, 0, 0, 3), ('near', 1, 0, 0, 1, 1), ('near', 2, 0, 1, 1, 2), ('partner', 1, 0, 0, 0, 0), ('partner', 1, 0, 0, 0, 2), ('partner', 1, 0, 0, 1, 0), ('near', 2, 1, 0, 0, 3), ('near', 1, 1, 0, 1, 3), ('near', 1, 1, 0, 1, 1), ('near', 2, 1, 0, 1, 3), ('near', 1, 0, 0, 1, 2), ('near', 2, 0, 1, 0, 0), ('near', 2, 0, 1, 1, 1), ('near', 1, 0, 0, 1, 3), ('near', 2, 1, 1, 1, 1), ('near', 2, 1, 1, 0, 0), ('near', 2, 1, 1, 0, 2), ('near', 2, 1, 1, 1, 2), ('near', 2, 0, 0, 1, 3), ('partner', 1, 0, 0, 1, 1), ('partner', 1, 0, 0, 1, 2), ('partner', 1, 0, 0, 0, 3), ('partner', 1, 0, 0, 1, 3), ('swap', 1), ('near', 2, 1, 1, 0, 3), ('near', 2, 1, 1, 1, 3), ('near', 2, 0, 1, 0, 2), ('near', 2, 0, 1, 1, 0), ('near', 2, 0, 1, 0, 3), ('near', 2, 0, 0, 1, 0), ('near', 2, 0, 1, 1, 3), ('near', 2, 0, 1, 0, 1), ('near', 2, 1, 1, 1, 0), ('near', 2, 1, 1, 0, 1), ('partner', 2, 0, 0, 0, 0), ('partner', 2, 0, 0, 0, 1), ('partner', 2, 0, 0, 0, 2), ('partner', 2, 0, 0, 0, 3), ('partner', 2, 0, 0, 1, 0), ('partner', 2, 0, 0, 1, 1), ('partner', 2, 0, 0, 1, 2), ('partner', 2, 0, 0, 1, 3), ('partner', 2, 0, 1, 0, 0), ('partner', 2, 0, 1, 0, 1), ('partner', 2, 0, 1, 0, 2), ('partner', 2, 0, 1, 0, 3), ('partner', 2, 0, 1, 1, 0), ('partner', 2, 0, 1, 1, 1), ('partner', 2, 0, 1, 1, 2), ('partner', 2, 0, 1, 1, 3)]}


def schedule(outer):
    return ORDERS[outer]


def nearest_first(outer):
    rows = []
    for z in range(outer):
        others = [q for q in range(outer) if q != z]
        others.sort(key=lambda q: (abs(q - z), q if 2 * z < outer else -q))
        rows.append([z] + others)
    return rows


def hops(kind, unit, r, yy, j):
    by_y, by_z = unit < ROUND_Y, unit < ROUND_Z
    if r == 1:
        if yy == 0 and j == 0:
            return ["y"] * by_y + ["up", "down"] * by_z
        return []
    ways = []
    if kind == 2:
        if yy == 1 and j == 0:
            ways += ["x"] * (not by_y)
        elif yy == 0 and j in (1, 2) and by_z:
            ways += ["x far"] * (j == 2)
        else:
            ways += ["x"]
    late = unit >= PIECES[kind] - SWAPPED[kind]
    if yy == 0 or late:
        ways += ["up", "down"] if j == 0 else ["on"]
    if yy == 0 and (j == 0 or not late):
        ways += ["y"]
    return ways


def part_of(kind, unit):
    return unit * PARTS[kind] // PIECES[kind]


def units_of(kind, part=None):
    if part is None:
        return range(PIECES[kind])
    return range(part * PIECES[kind] // PARTS[0], (part + 1) * PIECES[kind] // PARTS[0])


def sends_of(order):
    count, seen = 0, {}
    for what, kind, *rest in order:
        if what == "own":
            units = units_of(kind, *rest)
            count += sum(len(hops(kind, unit, 0, 0, 0)) for unit in units)
            count += len(rest) or PARTS[kind]
        elif what == "near":
            key = (kind, part_of(kind, rest[0]), *rest[1:])
            seen[key] = seen.get(key, 0) + 1
            count += len(hops(kind, *rest)) + (seen[key] == PIECES[kind] // PARTS[kind])
    return count


def gather_kernel(
    outer, order, acts, grads, a_hbm, g_hbm, pre, grad_pre,
    a_rows, g_rows, held, acc_a, acc_g,
    w_sem, send_sem, recv, recv_pre, x_recv, own_sem,
):
    group, width = acts.shape
    zero = outer * 4
    rep = lax.axis_index("rep")
    me = lax.axis_index("zero")
    z, y, c = me // 4, (me // 2) % 2, me % 2

    own = [
        pltpu.make_async_copy(acts, held.at[0, me], own_sem.at[0]),
        pltpu.make_async_copy(grads, held.at[1, me], own_sem.at[1]),
    ]
    loads = [
        pltpu.make_async_copy(a_hbm, a_rows, w_sem.at[0]),
        pltpu.make_async_copy(g_hbm, g_rows, w_sem.at[1]),
    ]
    own[0].start()
    own[1].start()

    x_peer = (1 - rep, me)
    y_peer = (rep, z * 4 + (1 - y) * 2 + c)
    c_peer = (rep, z * 4 + y * 2 + 1 - c)
    has_up, has_down = z < outer - 1, z > 0

    def z_peer(to):
        return (rep, to * 4 + y * 2 + c)

    barrier = pltpu.get_barrier_semaphore()

    def greet(peer):
        pl.semaphore_signal(barrier, inc=1, device_id=peer, device_id_type=MESH)

    for peer in (x_peer, y_peer, c_peer):
        greet(peer)
    pl.when(has_up)(lambda: greet(z_peer(z + 1)))
    pl.when(has_down)(lambda: greet(z_peer(z - 1)))
    pl.semaphore_wait(barrier, 3 + has_up.astype(jnp.int32) + has_down.astype(jnp.int32))

    table = nearest_first(outer)
    at_z = []
    for j in range(outer):
        value = jnp.int32(table[0][j])
        for q in range(1, outer):
            value = jnp.where(z == q, table[q][j], value)
        at_z.append(value)

    def block_of(kind, r, yy, j, other=False):
        cc = 1 - c if other else c
        block = at_z[j] * 4 + ((y + yy) % 2) * 2 + cc
        if kind == 2:
            block += ((rep + r) % 2) * zero
        return block

    def view(kind, block, unit=None):
        ref = pre.at[block] if kind == 2 else held.at[kind, block]
        if unit is None:
            return ref
        rows = group // PIECES[kind]
        return ref.at[pl.ds(unit * rows, rows)]

    def part_view(kind, block, part):
        if PARTS[kind] == 1:
            return view(kind, block)
        rows = group // PARTS[kind]
        return view(kind, block).at[pl.ds(part * rows, rows)]

    def landing(kind, block, unit):
        return recv_pre.at[block, unit] if kind == 2 else recv.at[kind, block, unit]

    sent = []

    def send(ref, peer, arrival, when=None):
        copy = pltpu.make_async_remote_copy(
            src_ref=ref, dst_ref=ref,
            send_sem=send_sem.at[len(sent)], recv_sem=arrival,
            device_id=peer, device_id_type=MESH,
        )
        sent.append((copy, when))
        if when is None:
            copy.start()
        else:
            pl.when(when)(copy.start)

    def forward(kind, unit, r, yy, j):
        block = block_of(kind, r, yy, j)
        ref, arrival = view(kind, block, unit), landing(kind, block, unit)
        onward = jnp.where(at_z[j] < z, z + 1, z - 1)
        ways = {
            "x": (x_peer, None),
            "x far": (x_peer, jnp.abs(at_z[j] - z) > 1),
            "y": (y_peer, None),
            "up": (z_peer(z + 1), has_up),
            "down": (z_peer(z - 1), has_down),
            "on": (z_peer(onward), (onward >= 0) & (onward < outer)),
        }
        for way in hops(kind, unit, r, yy, j):
            peer, when = ways[way]
            send(ref, peer, arrival, when)

    def to_partner(kind, part, r, yy, j):
        block = block_of(kind, r, yy, j)
        send(part_view(kind, block, part), c_peer, landing(kind, block, part))

    begun = [False] * 3
    waiting = [[], [], []]

    def catch_up(lot, count):
        kind = 1 if lot == PARTS[0] else 0
        if waiting[lot] and not any(begun[:2] if kind == 0 else begun[2:]):
            loads[kind].wait()
            if kind == 0:
                loads[1].start()
        for block in waiting[lot][:count]:
            add(lot, kind, block)
        del waiting[lot][:count]

    def add(lot, kind, block):
        columns = pl.ds(pl.multiple_of(block * width, width), width)
        if kind == 0:
            rows = group // PARTS[0]
            span = pl.ds(lot * rows, rows)
            acc = acc_a.at[span]
            term = lax.dot_general(
                held[0, block, span], a_rows[:, columns], NT, preferred_element_type=jnp.float32
            )
        else:
            acc = acc_g
            term = lax.dot_general(
                g_rows[:, columns], held[1, block], NT, preferred_element_type=jnp.float32
            )
        if begun[lot]:
            acc[...] += term
        else:
            acc[...] = term
            begun[lot] = True

    def wait(ref, arrival):
        pltpu.make_async_copy(ref, ref, arrival).wait()

    mine = rep * zero + me
    arrived = {}
    swap = pltpu.make_async_remote_copy(
        src_ref=grad_pre.at[rep], dst_ref=grad_pre.at[rep],
        send_sem=own_sem.at[2], recv_sem=x_recv,
        device_id=x_peer, device_id_type=MESH,
    )
    grad_lot = PARTS[0]
    for place, step in enumerate(order):
        what, kind = step[0], step[1]
        if place > HOLD:
            lot = next((q for q in range(grad_lot + 1) if waiting[q]), grad_lot)
            catch_up(lot, 2 if lot < grad_lot else 1)
        if what == "own":
            if kind == 2:
                part = step[2]
                catch_up(part, len(waiting[part]))
                rows = group // PARTS[0]
                span = pl.ds(part * rows, rows)
                pre[mine, span] = acc_a[span].astype(jnp.bfloat16)
            else:
                own[kind].wait()
            units = units_of(*step[1:])
            for unit in units:
                forward(kind, unit, 0, 0, 0)
            for part in step[2:] or range(PARTS[kind]):
                to_partner(kind, part, 0, 0, 0)
            if kind == 0:
                loads[0].start()
                for part in range(PARTS[0]):
                    waiting[part].append(me)
            elif kind == 1:
                waiting[grad_lot].append(me)
        elif what == "near":
            _, _, unit, r, yy, j = step
            block = block_of(kind, r, yy, j)
            wait(view(kind, block, unit), landing(kind, block, unit))
            forward(kind, unit, r, yy, j)
            part = part_of(kind, unit)
            key = (kind, part, r, yy, j)
            arrived[key] = arrived.get(key, 0) + 1
            if arrived[key] == PIECES[kind] // PARTS[kind]:
                to_partner(kind, part, r, yy, j)
                if kind < 2:
                    waiting[part if kind == 0 else grad_lot].append(block)
        elif what == "partner":
            _, _, part, r, yy, j = step
            block = block_of(kind, r, yy, j, True)
            for half in range(PARTS[2]) if kind == 2 else [part]:
                wait(part_view(kind, block, half), landing(kind, block, half))
            if kind < 2:
                waiting[part if kind == 0 else grad_lot].append(block)
        else:
            catch_up(grad_lot, len(waiting[grad_lot]))
            grad_pre[rep] = acc_g[...].astype(jnp.bfloat16)
            swap.start()
    swap.wait()
    for copy, when in sent:
        if when is None:
            copy.wait_send()
        else:
            pl.when(when)(copy.wait_send)


SLOTS = 4


def product_kernel(grad_ref, act_ref, out_hbm, tiles, sems):
    reps, zero, group, width = act_ref.shape
    tokens = reps * group
    rows = jnp.concatenate([grad_ref[r] for r in range(reps)], axis=1)
    copies = []
    for i in range(zero):
        slot = i % SLOTS
        if i >= SLOTS:
            copies[i - SLOTS].wait()
        block = jnp.concatenate([act_ref[r, i] for r in range(reps)], axis=0)
        summed = jnp.dot(rows, block, preferred_element_type=jnp.float32)
        if tokens & (tokens - 1):
            tiles[slot] = summed / jnp.float32(tokens)
        else:
            tiles[slot] = summed * jnp.float32(1 / tokens)
        copy = pltpu.make_async_copy(
            tiles.at[slot], out_hbm.at[:, pl.ds(i * width, width)], sems.at[slot]
        )
        copy.start()
        copies.append(copy)
    for copy in copies[-SLOTS:]:
        copy.wait()


def fused(acts, grads_out, act_inverse, grad_inverse):
    group, width = acts.shape
    zero = lax.axis_size("zero")
    reps = lax.axis_size("rep")
    rows, cols = act_inverse.shape
    outer = zero // 4
    bf16, dma = jnp.bfloat16, pltpu.SemaphoreType.DMA
    vmem = pl.BlockSpec(memory_space=pltpu.VMEM)
    hbm = pl.BlockSpec(memory_space=pltpu.HBM)
    order = schedule(outer)
    act_pre, grad_pre = pl.pallas_call(
        functools.partial(gather_kernel, outer, order),
        out_shape=(
            jax.ShapeDtypeStruct((reps * zero, group, width), bf16),
            jax.ShapeDtypeStruct((reps, width, group), bf16),
        ),
        in_specs=[hbm, hbm, hbm, hbm],
        out_specs=(vmem, vmem),
        scratch_shapes=[
            pltpu.VMEM((rows, cols), bf16),
            pltpu.VMEM((rows, cols), bf16),
            pltpu.VMEM((2, zero, group, width), bf16),
            pltpu.VMEM((group, width), jnp.float32),
            pltpu.VMEM((width, group), jnp.float32),
            dma((2,)),
            dma((sends_of(order),)),
            dma((2, zero, max(PIECES[:2]))),
            dma((reps * zero, PIECES[2])),
            dma,
            dma((3,)),
        ],
        compiler_params=pltpu.CompilerParams(
            collective_id=0, has_side_effects=True, vmem_limit_bytes=KERNEL_VMEM
        ),
    )(*(pltpu.with_memory_space_constraint(a, pltpu.HBM) for a in (acts, grads_out, act_inverse, grad_inverse)))
    return pl.pallas_call(
        product_kernel,
        out_shape=jax.ShapeDtypeStruct((rows, cols), jnp.float32),
        in_specs=[vmem, vmem],
        out_specs=hbm,
        scratch_shapes=[pltpu.VMEM((SLOTS, rows, width), jnp.float32), dma((SLOTS,))],
        compiler_params=pltpu.CompilerParams(vmem_limit_bytes=32 * 1024 * 1024),
    )(grad_pre, act_pre.reshape(reps, zero, group, width))


def on_device(acts, grads_out, act_inverse, grad_inverse):
    whole = acts.shape[1] % 128 == 0 and acts.shape[0] % 128 == 0
    if whole and lax.axis_size("rep") == 2 and lax.axis_size("zero") // 4 in ORDERS and lax.axis_size("zero") % 4 == 0:
        return fused(acts, grads_out, act_inverse, grad_inverse)
    return gathered(acts, grads_out, act_inverse, grad_inverse)


def solution(mesh):
    return jax.shard_map(
        on_device,
        mesh=mesh,
        in_specs=(P("rep", "zero"), P("rep", "zero"), P("zero", None), P("zero", None)),
        out_specs=P("zero", None),
        check_vma=False,
    )
```

```python
import functools

import jax
import jax.numpy as jnp
from jax import lax
from jax.experimental import pallas as pl
from jax.experimental.pallas import tpu as pltpu
from jax.sharding import PartitionSpec as P

NT = (((1,), (1,)), ((), ()))


def gathered(acts, grads_out, act_inverse, grad_inverse):
    group = acts.shape[0]
    total_tokens = group * lax.axis_size("rep")
    both = lax.all_gather(jnp.concatenate([acts, grads_out], 0), "zero", axis=1, tiled=True)
    act_own = lax.dot_general(
        both[:group], act_inverse, NT, preferred_element_type=jnp.float32
    ).astype(jnp.bfloat16)
    act_pre = lax.all_gather(act_own, ("rep", "zero"), axis=0)
    grad_own = lax.dot_general(
        both[group:], grad_inverse, NT, preferred_element_type=jnp.float32
    ).astype(jnp.bfloat16)
    grad_pre = lax.all_gather(grad_own, "rep", axis=0, tiled=True)
    zero = lax.axis_size("zero")
    act_pre = act_pre.reshape(-1, zero, group, act_own.shape[1]).transpose(0, 2, 1, 3)
    act_pre = act_pre.reshape(total_tokens, -1)
    summed = lax.dot_general(
        grad_pre, act_pre, (((0,), (0,)), ((), ())), preferred_element_type=jnp.float32
    )
    return summed / jnp.float32(total_tokens)


MESH = pl.DeviceIdType.MESH

PIECES = (4, 2, 2)
SWAPPED = (0, 0, 1)
ROUND_Y, ROUND_Z = 2, 1
HOLD = 8
PARTS = (2, 1, 1)
KERNEL_VMEM = 46137344

ORDERS = {4: [('own', 0), ('near', 0, 0, 0, 0, 1), ('near', 0, 1, 0, 0, 1), ('near', 0, 1, 0, 1, 0), ('near', 0, 0, 0, 1, 0), ('near', 0, 2, 0, 0, 1), ('near', 0, 1, 0, 0, 2), ('near', 0, 0, 0, 0, 2), ('near', 0, 3, 0, 0, 1), ('near', 0, 0, 0, 1, 1), ('near', 0, 0, 0, 0, 3), ('near', 0, 1, 0, 0, 3), ('partner', 0, 0, 0, 0, 1), ('near', 0, 1, 0, 1, 1), ('near', 0, 3, 0, 0, 2), ('partner', 0, 0, 0, 1, 0), ('near', 0, 1, 0, 1, 2), ('near', 0, 3, 0, 1, 0), ('near', 0, 2, 0, 0, 2), ('near', 0, 2, 0, 0, 3), ('partner', 0, 1, 0, 0, 1), ('partner', 0, 0, 0, 0, 2), ('near', 0, 3, 0, 0, 3), ('own', 1), ('near', 0, 2, 0, 1, 0), ('near', 0, 2, 0, 1, 1), ('near', 0, 3, 0, 1, 1), ('partner', 0, 1, 0, 0, 0), ('partner', 0, 0, 0, 1, 1), ('near', 0, 0, 0, 1, 3), ('partner', 0, 0, 0, 0, 3), ('near', 0, 0, 0, 1, 2), ('partner', 0, 0, 0, 0, 0), ('near', 0, 1, 0, 1, 3), ('partner', 0, 1, 0, 0, 3), ('partner', 0, 0, 0, 1, 2), ('partner', 0, 1, 0, 0, 2), ('partner', 0, 0, 0, 1, 3), ('near', 0, 3, 0, 1, 2), ('partner', 0, 1, 0, 1, 0), ('own', 2, 0), ('near', 0, 2, 0, 1, 2), ('partner', 0, 1, 0, 1, 1), ('near', 0, 3, 0, 1, 3), ('near', 0, 2, 0, 1, 3), ('partner', 0, 1, 0, 1, 2), ('near', 1, 1, 0, 0, 2), ('partner', 0, 1, 0, 1, 3), ('own', 2, 1), ('near', 2, 0, 0, 0, 2), ('near', 1, 0, 0, 1, 0), ('near', 1, 1, 0, 0, 1), ('near', 2, 1, 0, 0, 2), ('near', 2, 0, 0, 0, 1), ('near', 1, 1, 0, 0, 3), ('near', 2, 1, 0, 1, 0), ('near', 2, 1, 0, 0, 1), ('near', 2, 0, 0, 1, 2), ('near', 1, 1, 0, 1, 0), ('near', 1, 0, 0, 0, 1), ('near', 2, 0, 0, 0, 3), ('near', 2, 1, 0, 1, 2), ('near', 2, 0, 0, 1, 1), ('near', 1, 0, 0, 0, 2), ('near', 2, 1, 0, 1, 1), ('partner', 1, 0, 0, 0, 1), ('near', 1, 1, 0, 1, 2), ('near', 1, 0, 0, 0, 3), ('near', 1, 0, 0, 1, 1), ('near', 2, 0, 1, 1, 2), ('partner', 1, 0, 0, 0, 0), ('partner', 1, 0, 0, 0, 2), ('partner', 1, 0, 0, 1, 0), ('near', 2, 1, 0, 0, 3), ('near', 1, 1, 0, 1, 3), ('near', 1, 1, 0, 1, 1), ('near', 2, 1, 0, 1, 3), ('near', 1, 0, 0, 1, 2), ('near', 2, 0, 1, 0, 0), ('near', 2, 0, 1, 1, 1), ('near', 1, 0, 0, 1, 3), ('near', 2, 1, 1, 1, 1), ('near', 2, 1, 1, 0, 0), ('near', 2, 1, 1, 0, 2), ('near', 2, 1, 1, 1, 2), ('near', 2, 0, 0, 1, 3), ('partner', 1, 0, 0, 1, 1), ('partner', 1, 0, 0, 1, 2), ('partner', 1, 0, 0, 0, 3), ('partner', 1, 0, 0, 1, 3), ('swap', 1), ('near', 2, 1, 1, 0, 3), ('near', 2, 1, 1, 1, 3), ('near', 2, 0, 1, 0, 2), ('near', 2, 0, 1, 1, 0), ('near', 2, 0, 1, 0, 3), ('near', 2, 0, 0, 1, 0), ('near', 2, 0, 1, 1, 3), ('near', 2, 0, 1, 0, 1), ('near', 2, 1, 1, 1, 0), ('near', 2, 1, 1, 0, 1), ('partner', 2, 0, 0, 0, 0), ('partner', 2, 0, 0, 0, 1), ('partner', 2, 0, 0, 0, 2), ('partner', 2, 0, 0, 0, 3), ('partner', 2, 0, 0, 1, 0), ('partner', 2, 0, 0, 1, 1), ('partner', 2, 0, 0, 1, 2), ('partner', 2, 0, 0, 1, 3), ('partner', 2, 0, 1, 0, 0), ('partner', 2, 0, 1, 0, 1), ('partner', 2, 0, 1, 0, 2), ('partner', 2, 0, 1, 0, 3), ('partner', 2, 0, 1, 1, 0), ('partner', 2, 0, 1, 1, 1), ('partner', 2, 0, 1, 1, 2), ('partner', 2, 0, 1, 1, 3)]}


def schedule(outer):
    return ORDERS[outer]


def nearest_first(outer):
    rows = []
    for z in range(outer):
        others = [q for q in range(outer) if q != z]
        others.sort(key=lambda q: (abs(q - z), q if 2 * z < outer else -q))
        rows.append([z] + others)
    return rows


def hops(kind, unit, r, yy, j):
    by_y, by_z = unit < ROUND_Y, unit < ROUND_Z
    if r == 1:
        if yy == 0 and j == 0:
            return ["y"] * by_y + ["up", "down"] * by_z
        return []
    ways = []
    if kind == 2:
        if yy == 1 and j == 0:
            ways += ["x"] * (not by_y)
        elif yy == 0 and j in (1, 2) and by_z:
            ways += ["x far"] * (j == 2)
        else:
            ways += ["x"]
    late = unit >= PIECES[kind] - SWAPPED[kind]
    if yy == 0 or late:
        ways += ["up", "down"] if j == 0 else ["on"]
    if yy == 0 and (j == 0 or not late):
        ways += ["y"]
    return ways


def part_of(kind, unit):
    return unit * PARTS[kind] // PIECES[kind]


def units_of(kind, part=None):
    if part is None:
        return range(PIECES[kind])
    return range(part * PIECES[kind] // PARTS[0], (part + 1) * PIECES[kind] // PARTS[0])


def sends_of(order):
    count, seen = 0, {}
    for what, kind, *rest in order:
        if what == "own":
            units = units_of(kind, *rest)
            count += sum(len(hops(kind, unit, 0, 0, 0)) for unit in units)
            count += PARTS[kind] if kind == 0 else PIECES[kind] - 1 in units
        elif what == "near":
            key = (kind, part_of(kind, rest[0]), *rest[1:])
            seen[key] = seen.get(key, 0) + 1
            count += len(hops(kind, *rest)) + (seen[key] == PIECES[kind] // PARTS[kind])
    return count


def gather_kernel(
    outer, order, acts, grads, a_hbm, g_hbm, pre, grad_pre,
    a_rows, g_rows, held, acc_a, acc_g,
    w_sem, send_sem, recv, recv_pre, x_recv, own_sem,
):
    group, width = acts.shape
    zero = outer * 4
    rep = lax.axis_index("rep")
    me = lax.axis_index("zero")
    z, y, c = me // 4, (me // 2) % 2, me % 2

    own = [
        pltpu.make_async_copy(acts, held.at[0, me], own_sem.at[0]),
        pltpu.make_async_copy(grads, held.at[1, me], own_sem.at[1]),
    ]
    loads = [
        pltpu.make_async_copy(a_hbm, a_rows, w_sem.at[0]),
        pltpu.make_async_copy(g_hbm, g_rows, w_sem.at[1]),
    ]
    own[0].start()
    own[1].start()

    x_peer = (1 - rep, me)
    y_peer = (rep, z * 4 + (1 - y) * 2 + c)
    c_peer = (rep, z * 4 + y * 2 + 1 - c)
    has_up, has_down = z < outer - 1, z > 0

    def z_peer(to):
        return (rep, to * 4 + y * 2 + c)

    barrier = pltpu.get_barrier_semaphore()

    def greet(peer):
        pl.semaphore_signal(barrier, inc=1, device_id=peer, device_id_type=MESH)

    for peer in (x_peer, y_peer, c_peer):
        greet(peer)
    pl.when(has_up)(lambda: greet(z_peer(z + 1)))
    pl.when(has_down)(lambda: greet(z_peer(z - 1)))
    pl.semaphore_wait(barrier, 3 + has_up.astype(jnp.int32) + has_down.astype(jnp.int32))

    table = nearest_first(outer)
    at_z = []
    for j in range(outer):
        value = jnp.int32(table[0][j])
        for q in range(1, outer):
            value = jnp.where(z == q, table[q][j], value)
        at_z.append(value)

    def block_of(kind, r, yy, j, other=False):
        cc = 1 - c if other else c
        block = at_z[j] * 4 + ((y + yy) % 2) * 2 + cc
        if kind == 2:
            block += ((rep + r) % 2) * zero
        return block

    def view(kind, block, unit=None):
        ref = pre.at[block] if kind == 2 else held.at[kind, block]
        if unit is None:
            return ref
        rows = group // PIECES[kind]
        return ref.at[pl.ds(unit * rows, rows)]

    def part_view(kind, block, part):
        if PARTS[kind] == 1:
            return view(kind, block)
        rows = group // PARTS[kind]
        return held.at[kind, block, pl.ds(part * rows, rows)]

    def landing(kind, block, unit):
        return recv_pre.at[block, unit] if kind == 2 else recv.at[kind, block, unit]

    sent = []

    def send(ref, peer, arrival, when=None):
        copy = pltpu.make_async_remote_copy(
            src_ref=ref, dst_ref=ref,
            send_sem=send_sem.at[len(sent)], recv_sem=arrival,
            device_id=peer, device_id_type=MESH,
        )
        sent.append((copy, when))
        if when is None:
            copy.start()
        else:
            pl.when(when)(copy.start)

    def forward(kind, unit, r, yy, j):
        block = block_of(kind, r, yy, j)
        ref, arrival = view(kind, block, unit), landing(kind, block, unit)
        onward = jnp.where(at_z[j] < z, z + 1, z - 1)
        ways = {
            "x": (x_peer, None),
            "x far": (x_peer, jnp.abs(at_z[j] - z) > 1),
            "y": (y_peer, None),
            "up": (z_peer(z + 1), has_up),
            "down": (z_peer(z - 1), has_down),
            "on": (z_peer(onward), (onward >= 0) & (onward < outer)),
        }
        for way in hops(kind, unit, r, yy, j):
            peer, when = ways[way]
            send(ref, peer, arrival, when)

    def to_partner(kind, part, r, yy, j):
        block = block_of(kind, r, yy, j)
        send(part_view(kind, block, part), c_peer, landing(kind, block, part))

    begun = [False] * 3
    waiting = [[], [], []]

    def catch_up(lot, count):
        kind = 1 if lot == PARTS[0] else 0
        if waiting[lot] and not any(begun[:2] if kind == 0 else begun[2:]):
            loads[kind].wait()
            if kind == 0:
                loads[1].start()
        for block in waiting[lot][:count]:
            add(lot, kind, block)
        del waiting[lot][:count]

    def add(lot, kind, block):
        columns = pl.ds(pl.multiple_of(block * width, width), width)
        if kind == 0:
            rows = group // PARTS[0]
            span = pl.ds(lot * rows, rows)
            acc = acc_a.at[span]
            term = lax.dot_general(
                held[0, block, span], a_rows[:, columns], NT, preferred_element_type=jnp.float32
            )
        else:
            acc = acc_g
            term = lax.dot_general(
                g_rows[:, columns], held[1, block], NT, preferred_element_type=jnp.float32
            )
        if begun[lot]:
            acc[...] += term
        else:
            acc[...] = term
            begun[lot] = True

    def wait(ref, arrival):
        pltpu.make_async_copy(ref, ref, arrival).wait()

    mine = rep * zero + me
    arrived = {}
    swap = pltpu.make_async_remote_copy(
        src_ref=grad_pre.at[rep], dst_ref=grad_pre.at[rep],
        send_sem=own_sem.at[2], recv_sem=x_recv,
        device_id=x_peer, device_id_type=MESH,
    )
    grad_lot = PARTS[0]
    for place, step in enumerate(order):
        what, kind = step[0], step[1]
        if place > HOLD:
            lot = next((q for q in range(grad_lot + 1) if waiting[q]), grad_lot)
            catch_up(lot, 2 if lot < grad_lot else 1)
        if what == "own":
            if kind == 2:
                part = step[2]
                catch_up(part, len(waiting[part]))
                rows = group // PARTS[0]
                span = pl.ds(part * rows, rows)
                pre[mine, span] = acc_a[span].astype(jnp.bfloat16)
            else:
                own[kind].wait()
            units = units_of(*step[1:])
            for unit in units:
                forward(kind, unit, 0, 0, 0)
            if kind < 2 or PIECES[kind] - 1 in units:
                for part in range(PARTS[kind]):
                    to_partner(kind, part, 0, 0, 0)
            if kind == 0:
                loads[0].start()
                for part in range(PARTS[0]):
                    waiting[part].append(me)
            elif kind == 1:
                waiting[grad_lot].append(me)
        elif what == "near":
            _, _, unit, r, yy, j = step
            block = block_of(kind, r, yy, j)
            wait(view(kind, block, unit), landing(kind, block, unit))
            forward(kind, unit, r, yy, j)
            part = part_of(kind, unit)
            key = (kind, part, r, yy, j)
            arrived[key] = arrived.get(key, 0) + 1
            if arrived[key] == PIECES[kind] // PARTS[kind]:
                to_partner(kind, part, r, yy, j)
                if kind < 2:
                    waiting[part if kind == 0 else grad_lot].append(block)
        elif what == "partner":
            _, _, part, r, yy, j = step
            block = block_of(kind, r, yy, j, True)
            wait(part_view(kind, block, part), landing(kind, block, part))
            if kind < 2:
                waiting[part if kind == 0 else grad_lot].append(block)
        else:
            catch_up(grad_lot, len(waiting[grad_lot]))
            grad_pre[rep] = acc_g[...].astype(jnp.bfloat16)
            swap.start()
    swap.wait()
    for copy, when in sent:
        if when is None:
            copy.wait_send()
        else:
            pl.when(when)(copy.wait_send)


SLOTS = 8


def product_kernel(grad_ref, act_ref, out_hbm, tiles, sems):
    reps, zero, group, width = act_ref.shape
    tokens = reps * group
    rows = jnp.concatenate([grad_ref[r] for r in range(reps)], axis=1)
    copies = []
    for i in range(zero):
        slot = i % SLOTS
        if i >= SLOTS:
            copies[i - SLOTS].wait()
        block = jnp.concatenate([act_ref[r, i] for r in range(reps)], axis=0)
        summed = jnp.dot(rows, block, preferred_element_type=jnp.float32)
        if tokens & (tokens - 1):
            tiles[slot] = summed / jnp.float32(tokens)
        else:
            tiles[slot] = summed * jnp.float32(1 / tokens)
        copy = pltpu.make_async_copy(
            tiles.at[slot], out_hbm.at[:, pl.ds(i * width, width)], sems.at[slot]
        )
        copy.start()
        copies.append(copy)
    for copy in copies[-SLOTS:]:
        copy.wait()


def fused(acts, grads_out, act_inverse, grad_inverse):
    group, width = acts.shape
    zero = lax.axis_size("zero")
    reps = lax.axis_size("rep")
    rows, cols = act_inverse.shape
    outer = zero // 4
    bf16, dma = jnp.bfloat16, pltpu.SemaphoreType.DMA
    vmem = pl.BlockSpec(memory_space=pltpu.VMEM)
    hbm = pl.BlockSpec(memory_space=pltpu.HBM)
    order = schedule(outer)
    act_pre, grad_pre = pl.pallas_call(
        functools.partial(gather_kernel, outer, order),
        out_shape=(
            jax.ShapeDtypeStruct((reps * zero, group, width), bf16),
            jax.ShapeDtypeStruct((reps, width, group), bf16),
        ),
        in_specs=[hbm, hbm, hbm, hbm],
        out_specs=(vmem, vmem),
        scratch_shapes=[
            pltpu.VMEM((rows, cols), bf16),
            pltpu.VMEM((rows, cols), bf16),
            pltpu.VMEM((2, zero, group, width), bf16),
            pltpu.VMEM((group, width), jnp.float32),
            pltpu.VMEM((width, group), jnp.float32),
            dma((2,)),
            dma((sends_of(order),)),
            dma((2, zero, max(PIECES[:2]))),
            dma((reps * zero, PIECES[2])),
            dma,
            dma((3,)),
        ],
        compiler_params=pltpu.CompilerParams(
            collective_id=0, has_side_effects=True, vmem_limit_bytes=KERNEL_VMEM
        ),
    )(*(pltpu.with_memory_space_constraint(a, pltpu.HBM) for a in (acts, grads_out, act_inverse, grad_inverse)))
    return pl.pallas_call(
        product_kernel,
        out_shape=jax.ShapeDtypeStruct((rows, cols), jnp.float32),
        in_specs=[vmem, vmem],
        out_specs=hbm,
        scratch_shapes=[pltpu.VMEM((SLOTS, rows, width), jnp.float32), dma((SLOTS,))],
        compiler_params=pltpu.CompilerParams(vmem_limit_bytes=32 * 1024 * 1024),
    )(grad_pre, act_pre.reshape(reps, zero, group, width))


def on_device(acts, grads_out, act_inverse, grad_inverse):
    whole = acts.shape[1] % 128 == 0 and acts.shape[0] % 128 == 0
    if whole and lax.axis_size("rep") == 2 and lax.axis_size("zero") // 4 in ORDERS and lax.axis_size("zero") % 4 == 0:
        return fused(acts, grads_out, act_inverse, grad_inverse)
    return gathered(acts, grads_out, act_inverse, grad_inverse)


def solution(mesh):
    return jax.shard_map(
        on_device,
        mesh=mesh,
        in_specs=(P("rep", "zero"), P("rep", "zero"), P("zero", None), P("zero", None)),
        out_specs=P("zero", None),
        check_vma=False,
    )
```
